32 devices in a mesh: fsdp: 4 (over y, x), tensor: 8 (over z, core).
Axes of the slice: x: 2, y: 2, z: 4, core: 2. Of those that a mesh axis runs over, the one named last changes fastest.
Arguments:
- modality: int32 [4096], P('fsdp'), may hold values from 0 to 2, as said below
- out_grad: bfloat16 [4096, 4096], P('fsdp', 'tensor'), may hold values from -6 to 6
- gate_pre: bfloat16 [4096, 11008], P('fsdp', 'tensor'), may hold values from -6 to 6
- up_pre: bfloat16 [4096, 11008], P('fsdp', 'tensor'), may hold values from -6 to 6
- down_weight: bfloat16 [3, 11008, 4096], P(None, 'tensor', 'fsdp'), may hold values from -0.0546875 to 0.0546875
Outputs:
- down_grad: float32 [3, 11008, 4096], P(None, 'tensor', 'fsdp')
- gate_grad: bfloat16 [4096, 11008], P('fsdp', 'tensor')
- up_grad: bfloat16 [4096, 11008], P('fsdp', 'tensor')
The draws below stay inside these ranges and needn't reach their ends.
Inputs may be any that keep to these rules, and one draw needn't show every extreme that they name: `modality`: the 1024 tokens of every index of fsdp hold each of the three modalities at least once.
All inputs are finite; a program needn't handle non-finite values.
Results may differ from the reference program's by a relative error of at most 0.012.
Values may be sent and summed in bfloat16 or wider, within the bound.
A program may use at most 256 MiB of HBM per device.

```python
import jax
import jax.numpy as jnp
from jax import lax

D = 4096
FF = 11008
TOK_DEV = 1024
TOKENS = 4096
N_FSDP = 4


def draw_modality(key, part):
    subkeys = jax.random.split(jax.random.fold_in(key, 11), 4)
    groups = TOKENS // TOK_DEV
    position = jnp.arange(TOKENS, dtype=jnp.int32)
    group_id = position // TOK_DEV
    local_pos = position % TOK_DEV
    rotation = jax.random.randint(subkeys[0], (), 0, 3)
    leader = (jnp.arange(groups, dtype=jnp.int32) + rotation) % 3
    shares = jax.random.randint(subkeys[1], (groups,), 3, 9)
    offsets = jax.random.randint(subkeys[2], (groups,), 0, TOK_DEV)
    rolls = jax.random.randint(subkeys[3], (TOKENS,), 0, 20)
    lead_kind = leader[group_id]
    base_kind = jnp.where(rolls < 2 * shares[group_id], lead_kind, (lead_kind + 1 + rolls % 2) % 3)
    distance = (local_pos - offsets[group_id]) % TOK_DEV
    return jnp.where(distance < 3, distance, base_kind).astype(jnp.int32)


def spiked(entries, stream_key, source, target, shards_of, factor):
    owner, partner = [(jnp.arange(entries.shape[axis_at]) // (entries.shape[axis_at] // shards_of)).reshape([-1 if axis == axis_at else 1 for axis in range(entries.ndim)]) for axis_at in (source, target)]
    chosen = jax.random.permutation(stream_key, shards_of)[partner]
    strong = (owner == chosen) | (owner == (partner + shards_of // 2) % shards_of)
    return jnp.where(strong, factor * entries, entries)


def block_scale(rng, shape, pieces, smallest, high):
    def one(dim, shards_of):
        heights = jax.random.uniform(jax.random.fold_in(jax.random.fold_in(rng, 6), dim), (shards_of,), jnp.float32, smallest / len(pieces), high / len(pieces))
        return jnp.repeat(jnp.exp(heights), shape[dim] // shards_of).reshape((-1,) + (1,) * (len(shape) - dim - 1))

    factor_of = one(*pieces[0])
    for cut in pieces[1:]:
        factor_of = factor_of * one(*cut)
    return factor_of


def gaussian(stream_key, shape, deviation, bound, cuts=(), kind=jnp.bfloat16):
    loudness = block_scale(stream_key, shape, cuts, -0.22, 0.18) if cuts else 1.0
    drawn = jax.random.normal(stream_key, shape, jnp.float32) * deviation * loudness
    return jnp.minimum(jnp.maximum(drawn, -bound), bound).astype(kind)


def gaussian_with(own_key, dims, width, bound, cuts, heavy, kind=jnp.bfloat16):
    array = width * jax.random.normal(own_key, dims, jnp.float32)
    if cuts:
        array = array * block_scale(own_key, dims, cuts, -0.22, 0.18)
    return jnp.clip(spiked(array, jax.random.fold_in(own_key, 3), *heavy), -bound, bound).astype(kind)


def setup_inputs(seed: int = 0) -> dict:
    keys = jax.random.split(jax.random.key(seed), 6)
    modality = draw_modality(jax.random.fold_in(keys[5], 71), 0)
    out_grad = gaussian_with(keys[1], (TOKENS, D), 1.0, 6.0, ((0, 4), (1, 8)), (0, 1, 8, 2.0))
    gate_pre = gaussian(keys[2], (TOKENS, FF), 1.0, 6.0, ((0, 4), (1, 8)))
    up_pre = gaussian(keys[3], (TOKENS, FF), 1.0, 6.0, ((0, 4), (1, 8)))
    down_weight = gaussian(keys[4], (3, FF, D), FF ** -0.5, 0.0546875, ((1, 8), (2, 4)))
    return dict(modality=modality, out_grad=out_grad, gate_pre=gate_pre, up_pre=up_pre, down_weight=down_weight)


def reference(modality, out_grad, gate_pre, up_pre, down_weight):
    labels = jnp.arange(3, dtype=jnp.int32)
    kind_onehot = (modality[:, None] == labels[None, :]).astype(jnp.float32)
    counts = jnp.sum(kind_onehot, axis=0)
    factor = TOKENS / (3.0 * counts)
    token_scale = jnp.sum(kind_onehot * factor[None, :], axis=1)
    scaled = (out_grad.astype(jnp.float32) * token_scale[:, None]).astype(jnp.bfloat16)
    gate_val = gate_pre.astype(jnp.float32)
    up_val = up_pre.astype(jnp.float32)
    sigmoid_g = jax.nn.sigmoid(gate_val)
    active = gate_val * sigmoid_g
    hidden = (active * up_val).astype(jnp.bfloat16)
    kind_marks = kind_onehot.T.astype(jnp.bfloat16)
    d_hidden = jnp.zeros((TOKENS, FF), jnp.float32)
    for kind_id in range(3):
        masked = scaled * kind_marks[kind_id][:, None]
        d_hidden = d_hidden + lax.dot_general(masked, down_weight[kind_id], (((1,), (1,)), ((), ())), preferred_element_type=jnp.float32)
    up_grad = (d_hidden * active).astype(jnp.bfloat16)
    slope = sigmoid_g * (1.0 + gate_val * (1.0 - sigmoid_g))
    gate_grad = (d_hidden * up_val * slope).astype(jnp.bfloat16)
    group_hidden = hidden.reshape(N_FSDP, TOK_DEV, FF)
    group_scaled = scaled.reshape(N_FSDP, TOK_DEV, D)
    group_marks = jnp.transpose(kind_marks.reshape(3, N_FSDP, TOK_DEV), (1, 0, 2))

    def one_group(running, group_items):
        rows_hidden, rows_scaled, marks_here = group_items
        partials = []
        for kind_id in range(3):
            masked = rows_scaled * marks_here[kind_id][:, None]
            product = lax.dot_general(rows_hidden, masked, (((0,), (0,)), ((), ())), preferred_element_type=jnp.float32)
            partials.append(lax.optimization_barrier(product.astype(jnp.bfloat16)).astype(jnp.float32))
        return running + jnp.stack(partials), None

    down_grad, _ = lax.scan(one_group, jnp.zeros((3, FF, D), jnp.float32), (group_hidden, group_scaled, group_marks))
    return down_grad, gate_grad, up_grad
```

```python
import jax
import jax.numpy as jnp
from jax import lax
from jax.sharding import PartitionSpec as P


def kind_table(kind_ids):
    labels = jnp.arange(3, dtype=jnp.int32)
    return (kind_ids[:, None] == labels[None, :]).astype(jnp.float32)


def swap(values, axis, size, step):
    return lax.ppermute(values, axis, [(i, i ^ step) for i in range(size)])


def activations(gate_pre, up_pre):
    gate_val = gate_pre.astype(jnp.float32)
    up_val = up_pre.astype(jnp.float32)
    sigmoid_g = jax.nn.sigmoid(gate_val)
    return gate_val, up_val, sigmoid_g, gate_val * sigmoid_g


def hidden_of(gate_pre, up_pre):
    _, up_val, _, active = activations(gate_pre, up_pre)
    return (active * up_val).astype(jnp.bfloat16)


def grads_of(folded, gate_pre, up_pre):
    gate_val, up_val, sigmoid_g, active = activations(gate_pre, up_pre)
    up_grad = (folded * active).astype(jnp.bfloat16)
    slope = sigmoid_g * (1.0 + gate_val * (1.0 - sigmoid_g))
    gate_grad = (folded * up_val * slope).astype(jnp.bfloat16)
    return gate_grad, up_grad


def masked_back(scaled, onehot, down_weight):
    marks = onehot.T.astype(jnp.bfloat16)
    masked = scaled[None, :, :] * marks[:, :, None]
    return lax.dot_general(
        masked, down_weight, (((0, 2), (0, 2)), ((), ())), preferred_element_type=jnp.float32
    )


def weight_grad(hid_all, scaled_all, onehot_all):
    marks_all = onehot_all.T.astype(jnp.bfloat16)
    masked_all = scaled_all[None, :, :] * marks_all[:, :, None]
    stacked = jnp.broadcast_to(hid_all[None, :, :], (3,) + hid_all.shape)
    return lax.dot_general(
        stacked, masked_all, (((1,), (1,)), ((0,), (0,))), preferred_element_type=jnp.float32
    )


def shards_planes(modality, out_grad, gate_pre, up_pre, down_weight):
    rows, block = out_grad.shape
    groups = lax.axis_size("fsdp")
    lanes = lax.axis_size("tensor")
    planes = lanes // 2
    quarter = rows // planes
    half = rows // 2
    me = lax.axis_index("fsdp")
    lane = lax.axis_index("tensor")
    plane = lane // 2
    core = lane % 2

    kinds = [modality] + [swap(modality, "fsdp", groups, k) for k in range(1, groups)]

    own = out_grad.reshape(planes, quarter, block)
    legs = []
    for d in range(planes):
        part = lax.dynamic_index_in_dim(own, plane ^ d, 0, keepdims=False)
        legs.append(swap(part, "tensor", lanes, 2 * d) if d else part)

    hid_a = hidden_of(gate_pre[:half], up_pre[:half])
    hid_b = hidden_of(gate_pre[half:], up_pre[half:])
    hid1b = swap(hid_b, "fsdp", groups, 1)
    hid2a = swap(hid_a, "fsdp", groups, 2)

    stacked = jnp.stack(legs)
    crossed = {}
    for k in (3, 1, 2, 0):
        part = lax.dynamic_index_in_dim(stacked, plane ^ me ^ k, 0, keepdims=False)
        crossed[k] = swap(part, "fsdp", groups, k) if k else part

    hid1a = swap(hid_a, "fsdp", groups, 1)
    hid2b = swap(hid_b, "fsdp", groups, 2)
    hid3a = swap(hid2a, "fsdp", groups, 1)
    hid3b = swap(hid1b, "fsdp", groups, 2)

    onehots = [kind_table(kind_ids) for kind_ids in kinds]
    counts = sum(jnp.sum(onehot, axis=0) for onehot in onehots)
    factor = rows * groups / (3.0 * counts)

    odd = plane % 2 == 1
    upper = plane // 2 == 1
    inner = (plane == 1) | (plane == 2)
    middle = [(2 * p + c, 2 * (3 - p) + c) for p in (1, 2) for c in range(2)]
    outward = [(2 * p + c, 2 * (p ^ 1) + c) for p in (1, 2) for c in range(2)]
    scaled = {}
    for k in (3, 1, 2, 0):
        mine = crossed[k]
        near = swap(mine, "tensor", lanes, 2)
        pair = jnp.where(odd, jnp.concatenate([near, mine]), jnp.concatenate([mine, near]))
        across = lax.ppermute(pair, "tensor", middle)
        onward = lax.ppermute(across, "tensor", outward)
        beyond = jnp.where(inner, across, onward)
        part = jnp.where(upper, jnp.concatenate([beyond, pair]), jnp.concatenate([pair, beyond]))
        other = swap(part, "tensor", lanes, 1)
        joined = jnp.where(
            core == 0,
            jnp.concatenate([part, other], axis=1),
            jnp.concatenate([other, part], axis=1),
        )
        token_scale = jnp.sum(onehots[k] * factor[None, :], axis=1)
        scaled[k] = (joined.astype(jnp.float32) * token_scale[:, None]).astype(jnp.bfloat16)

    def back(k, lo, hi):
        return masked_back(scaled[k][lo:hi], onehots[k][lo:hi], down_weight)

    via1 = swap(back(3, 0, half).astype(jnp.bfloat16), "fsdp", groups, 1)
    via2 = swap(back(3, half, rows).astype(jnp.bfloat16), "fsdp", groups, 2)
    got1a = swap(back(1, 0, half).astype(jnp.bfloat16), "fsdp", groups, 1)
    got2b = swap(back(2, half, rows).astype(jnp.bfloat16), "fsdp", groups, 2)
    near2 = (back(2, 0, half) + via1.astype(jnp.float32)).astype(jnp.bfloat16)
    near1 = (back(1, half, rows) + via2.astype(jnp.float32)).astype(jnp.bfloat16)
    cut = half // 2
    got2a = [swap(near2[i : i + cut], "fsdp", groups, 2) for i in (0, cut)]
    got1b = [swap(near1[i : i + cut], "fsdp", groups, 1) for i in (0, cut)]

    base_a = back(0, 0, half) + got1a.astype(jnp.float32)
    base_b = back(0, half, rows) + got2b.astype(jnp.float32)
    base_a, base_b = lax.optimization_barrier((base_a, base_b))

    hid_all = jnp.concatenate([hid_a, hid_b, hid1a, hid1b, hid2a, hid2b, hid3a, hid3b], axis=0)
    scaled_all = jnp.concatenate([scaled[k] for k in range(groups)], axis=0)
    onehot_all = jnp.concatenate(onehots, axis=0)
    down_grad = weight_grad(hid_all, scaled_all, onehot_all)

    gates, ups = [], []
    for lo, base, got in (
        (0, base_a[:cut], got2a[0]),
        (cut, base_a[cut:], got2a[1]),
        (half, base_b[:cut], got1b[0]),
        (half + cut, base_b[cut:], got1b[1]),
    ):
        folded = base + got.astype(jnp.float32)
        gate_part, up_part = grads_of(folded, gate_pre[lo : lo + cut], up_pre[lo : lo + cut])
        gates.append(gate_part)
        ups.append(up_part)
    return (down_grad, jnp.concatenate(gates), jnp.concatenate(ups))


def shards(modality, out_grad, gate_pre, up_pre, down_weight):
    rows, block = out_grad.shape
    groups = lax.axis_size("fsdp")
    lanes = lax.axis_size("tensor")
    width = down_weight.shape[2]
    me = lax.axis_index("fsdp")
    core = lax.axis_index("tensor") % 2
    pieces = width // (2 * block)

    cores = [[i for i in range(lanes) if i % 2 == c] for c in range(2)]
    stripe = lax.all_gather(out_grad, "tensor", axis=0, axis_index_groups=cores)
    stripe = stripe.reshape(groups, pieces, rows, block)

    hidden = hidden_of(gate_pre, up_pre)
    hid_list = [hidden] + [swap(hidden, "fsdp", groups, k) for k in range(1, groups)]

    kinds = lax.all_gather(modality, "fsdp", axis=0)
    counts = jnp.sum(kind_table(kinds.reshape(-1)), axis=0)
    factor = rows * groups / (3.0 * counts)

    order = [groups - 1] + list(range(1, groups - 1)) + [0]
    onehots, scaled = {}, {}
    for k in order:
        part = lax.dynamic_index_in_dim(stripe, me ^ k, 0, keepdims=False)
        if k:
            part = swap(part, "fsdp", groups, k)
        other = swap(part, "tensor", lanes, 1)
        first = jnp.where(core == 0, part, other)
        second = jnp.where(core == 0, other, part)
        joined = jnp.stack([first, second], axis=1).reshape(2 * pieces, rows, block)
        joined = jnp.concatenate([joined[i] for i in range(2 * pieces)], axis=1)
        onehots[k] = kind_table(lax.dynamic_index_in_dim(kinds, me ^ k, 0, keepdims=False))
        token_scale = jnp.sum(onehots[k] * factor[None, :], axis=1)
        scaled[k] = (joined.astype(jnp.float32) * token_scale[:, None]).astype(jnp.bfloat16)

    folded = masked_back(scaled[0], onehots[0], down_weight)
    for k in range(1, groups):
        sent = masked_back(scaled[k], onehots[k], down_weight).astype(jnp.bfloat16)
        folded = folded + swap(sent, "fsdp", groups, k).astype(jnp.float32)
    gate_grad, up_grad = grads_of(folded, gate_pre, up_pre)

    hid_all = jnp.concatenate(hid_list, axis=0)
    scaled_all = jnp.concatenate([scaled[k] for k in range(groups)], axis=0)
    onehot_all = jnp.concatenate([onehots[k] for k in range(groups)], axis=0)
    down_grad = weight_grad(hid_all, scaled_all, onehot_all)
    return (down_grad, gate_grad, up_grad)


def solution(mesh):
    placed = (
        P("fsdp"),
        P("fsdp", "tensor"),
        P("fsdp", "tensor"),
        P("fsdp", "tensor"),
        P(None, "tensor", "fsdp"),
    )
    square = mesh.shape["fsdp"] == 4 and mesh.shape["tensor"] == 8
    return jax.shard_map(
        shards_planes if square else shards,
        mesh=mesh,
        in_specs=placed,
        out_specs=(P(None, "tensor", "fsdp"), P("fsdp", "tensor"), P("fsdp", "tensor")),
        check_vma=False,
    )
```

```python
import functools

import jax
import jax.numpy as jnp
from jax import lax
from jax.experimental import pallas as pl
from jax.experimental.pallas import tpu as pltpu
from jax.sharding import PartitionSpec as P


def kind_table(kind_ids):
    labels = jnp.arange(3, dtype=jnp.int32)
    return (kind_ids[:, None] == labels[None, :]).astype(jnp.float32)


def swap(values, axis, size, step):
    return lax.ppermute(values, axis, [(i, i ^ step) for i in range(size)])


def activations(gate_pre, up_pre):
    gate_val = gate_pre.astype(jnp.float32)
    up_val = up_pre.astype(jnp.float32)
    sigmoid_g = jax.nn.sigmoid(gate_val)
    return gate_val, up_val, sigmoid_g, gate_val * sigmoid_g


def hidden_of(gate_pre, up_pre):
    _, up_val, _, active = activations(gate_pre, up_pre)
    return (active * up_val).astype(jnp.bfloat16)


def grads_of(folded, gate_pre, up_pre):
    gate_val, up_val, sigmoid_g, active = activations(gate_pre, up_pre)
    up_grad = (folded * active).astype(jnp.bfloat16)
    slope = sigmoid_g * (1.0 + gate_val * (1.0 - sigmoid_g))
    gate_grad = (folded * up_val * slope).astype(jnp.bfloat16)
    return gate_grad, up_grad


def masked_back(scaled, onehot, down_weight):
    marks = onehot.T.astype(jnp.bfloat16)
    masked = scaled[None, :, :] * marks[:, :, None]
    return lax.dot_general(
        masked, down_weight, (((0, 2), (0, 2)), ((), ())), preferred_element_type=jnp.float32
    )


def weight_grad(hid_all, scaled_all, onehot_all):
    marks_all = onehot_all.T.astype(jnp.bfloat16)
    masked_all = scaled_all[None, :, :] * marks_all[:, :, None]
    stacked = jnp.broadcast_to(hid_all[None, :, :], (3,) + hid_all.shape)
    return lax.dot_general(
        stacked, masked_all, (((1,), (1,)), ((0,), (0,))), preferred_element_type=jnp.float32
    )


HBM = pltpu.MemorySpace.HBM


def weight_body(kinds, owners, tile, *refs):
    pieces = refs[: sum(len(owner) for owner in owners)]
    scaled = refs[len(pieces) : len(pieces) + len(owners)]
    marks_ref = refs[len(pieces) + len(owners)]
    out_ref, hid_buf, scaled_buf, total, hid_sem, scaled_sem, out_sem = refs[-7:]
    chunks = len(owners)
    tiles = total.shape[1] // tile

    def fetch(at, slot, act):
        for c, owner in enumerate(owners):

            @pl.when(at == c)
            def _():
                act(pltpu.make_async_copy(scaled[c], scaled_buf.at[slot], scaled_sem.at[slot]))
                for p, (index, offset, count) in enumerate(owner):
                    here = hid_buf.at[slot, :, pl.ds(offset, count)]
                    act(pltpu.make_async_copy(pieces[index], here, hid_sem.at[slot, p]))

    fetch(0, 0, lambda copy: copy.start())

    def columns(t):
        return pl.ds(pl.multiple_of(t * tile, tile), tile)

    def put(n, t):
        return pltpu.make_async_copy(
            total.at[:, columns(t)], out_ref.at[kinds[0] + n, :, columns(t)], out_sem.at[t]
        )

    def chunk(step, carry):
        n, c = step // chunks, lax.rem(step, chunks)
        slot = lax.rem(step, 2)

        @pl.when(step + 1 < len(kinds) * chunks)
        def _():
            fetch(lax.rem(step + 1, chunks), 1 - slot, lambda copy: copy.start())

        fetch(c, slot, lambda copy: copy.wait())

        def one(t, carry):
            @pl.when((c == 0) & (n > 0))
            def _():
                put(n - 1, t).wait()

            mark = marks_ref[n, c].astype(jnp.bfloat16)
            part = jnp.dot(
                hid_buf[slot] * mark,
                scaled_buf[slot, :, columns(t)],
                preferred_element_type=jnp.float32,
            )
            total[:, columns(t)] = jnp.where(c > 0, total[:, columns(t)], 0.0) + part

            @pl.when(c == chunks - 1)
            def _():
                put(n, t).start()

            return carry

        return lax.fori_loop(0, tiles, one, carry)

    lax.fori_loop(0, len(kinds) * chunks, chunk, 0)
    for t in range(tiles):
        put(len(kinds) - 1, t).wait()


def weight_grad_of(kinds, hidden, scaled, marks, before):
    owners, pieces = [], []
    for owner in hidden:
        listed, offset = [], 0
        for piece in owner:
            listed.append((len(pieces), offset, piece.shape[1]))
            pieces.append(piece)
            offset += piece.shape[1]
        owners.append(tuple(listed))
    rows, cols = scaled[0].shape
    width = pieces[0].shape[0]
    tiles = 2
    hbm = pl.BlockSpec(memory_space=HBM)
    operands = [*pieces, *scaled, marks]
    specs = [hbm] * (len(operands) - 1) + [pl.BlockSpec(memory_space=pltpu.VMEM)]
    aliases = {}
    if before is not None:
        operands.append(before)
        specs.append(hbm)
        aliases = {len(operands) - 1: 0}
    most = max(len(owner) for owner in owners)
    tokens = rows * len(owners)
    return pl.pallas_call(
        functools.partial(weight_body, kinds, tuple(owners), cols // tiles),
        out_shape=jax.ShapeDtypeStruct((3, width, cols), jnp.float32),
        in_specs=specs,
        out_specs=hbm,
        scratch_shapes=[
            pltpu.VMEM((2, width, rows), jnp.bfloat16),
            pltpu.VMEM((2, rows, cols), jnp.bfloat16),
            pltpu.VMEM((width, cols), jnp.float32),
            pltpu.SemaphoreType.DMA((2, most)),
            pltpu.SemaphoreType.DMA((2,)),
            pltpu.SemaphoreType.DMA((tiles,)),
        ],
        input_output_aliases=aliases,
        compiler_params=pltpu.CompilerParams(vmem_limit_bytes=24 * 2**20),
        cost_estimate=pl.CostEstimate(
            flops=2 * len(kinds) * tokens * width * cols,
            bytes_accessed=2 * tokens * (width + cols) + 4 * len(kinds) * width * cols,
            transcendentals=0,
        ),
    )(*operands)


def grads_body(base_ref, direct_ref, got_ref, gate_ref, up_ref, *refs):
    gate_out, up_out = refs[-2:]
    lane = 128

    def one(j, carry):
        at = (slice(None), pl.ds(pl.multiple_of(j * lane, lane), lane))
        folded = base_ref[at] + direct_ref[at].astype(jnp.float32) + got_ref[at].astype(jnp.float32)
        gate_out[at], up_out[at] = grads_of(folded, gate_ref[at], up_ref[at])
        return carry

    lax.fori_loop(0, got_ref.shape[1] // lane, one, 0)


def grads_into(base, direct, first, got, gate_turned, up_turned, column, before):
    width, count = got.shape
    steps = 4 if width % 64 == 0 else 1
    tall = width // steps

    def at(start):
        return pl.BlockSpec((tall, count), lambda i: (i, start // count))

    operands = [base, direct, got, gate_turned, up_turned]
    specs = [at(first), at(first), at(0), at(column), at(column)]
    aliases = {}
    if before is not None:
        operands += before
        specs += [pl.BlockSpec(memory_space=HBM)] * 2
        aliases = {5: 0, 6: 1}
    out = jax.ShapeDtypeStruct(gate_turned.shape, jnp.bfloat16)
    return pl.pallas_call(
        grads_body,
        grid=(steps,),
        out_shape=(out, out),
        in_specs=specs,
        out_specs=(at(column), at(column)),
        input_output_aliases=aliases,
        compiler_params=pltpu.CompilerParams(vmem_limit_bytes=16 * 2**20),
        cost_estimate=pl.CostEstimate(
            flops=20 * width * count,
            bytes_accessed=16 * width * count,
            transcendentals=width * count,
        ),
    )(*operands)


def shards_planes(modality, out_grad, gate_pre, up_pre, down_weight):
    return planes_body(modality, out_grad, gate_pre, up_pre, down_weight)


def planes_body(modality, out_grad, gate_pre, up_pre, down_weight):
    rows, block = out_grad.shape
    groups = lax.axis_size("fsdp")
    lanes = lax.axis_size("tensor")
    planes = lanes // 2
    quarter = rows // planes
    half = rows // 2
    cut = half // 2
    me = lax.axis_index("fsdp")
    lane = lax.axis_index("tensor")
    plane = lane // 2
    core = lane % 2
    gate_turned, up_turned = gate_pre.T, up_pre.T

    def over(values, step):
        return lax.ppermute(values, "fsdp", [(i, i ^ step) for i in range(groups)])

    def along(values, step):
        return lax.ppermute(values, "tensor", [(i, i ^ step) for i in range(lanes)])

    hid_a = hidden_of(gate_turned[:, :half], up_turned[:, :half])
    hid_b = hidden_of(gate_turned[:, half:], up_turned[:, half:])
    hid1b, hid2a = over(hid_b, 1), over(hid_a, 2)
    hid1a, hid2b = over(hid_a, 1), over(hid_b, 2)
    hid3a, hid3b = over(hid2a, 1), over(hid1b, 2)
    hidden = [[hid_a, hid_b], [hid1a, hid1b], [hid2a, hid2b], [hid3a, hid3b]]

    own = out_grad.reshape(planes, quarter, block)
    legs = []
    for d in range(planes):
        part = lax.dynamic_index_in_dim(own, plane ^ d, 0, keepdims=False)
        legs.append(along(part, 2 * d) if d else part)

    kinds = [modality] + [over(modality, k) for k in range(1, groups)]

    stacked = jnp.stack(legs)
    crossed = {}
    for k in (3, 1, 2, 0):
        part = lax.dynamic_index_in_dim(stacked, plane ^ me ^ k, 0, keepdims=False)
        crossed[k] = over(part, k) if k else part

    onehots = [kind_table(kind_ids) for kind_ids in kinds]
    counts = sum(jnp.sum(onehot, axis=0) for onehot in onehots)
    factor = rows * groups / (3.0 * counts)

    odd = plane % 2 == 1
    upper = plane // 2 == 1
    inner = (plane == 1) | (plane == 2)
    middle = [(2 * p + c, 2 * (3 - p) + c) for p in (1, 2) for c in range(2)]
    outward = [(2 * p + c, 2 * (p ^ 1) + c) for p in (1, 2) for c in range(2)]
    scaled = {}
    for k in (0, 3, 1, 2):
        mine = crossed[k]
        near = along(mine, 2)
        pair = jnp.where(odd, jnp.concatenate([near, mine]), jnp.concatenate([mine, near]))
        across = lax.ppermute(pair, "tensor", middle)
        onward = lax.ppermute(across, "tensor", outward)
        beyond = jnp.where(inner, across, onward)
        part = jnp.where(upper, jnp.concatenate([beyond, pair]), jnp.concatenate([pair, beyond]))
        other = along(part, 1)
        joined = jnp.where(
            core == 0,
            jnp.concatenate([part, other], axis=1),
            jnp.concatenate([other, part], axis=1),
        )
        token_scale = jnp.sum(onehots[k] * factor[None, :], axis=1)
        scaled[k] = (joined.astype(jnp.float32) * token_scale[:, None]).astype(jnp.bfloat16)

    def back(k, lo, hi):
        return masked_back(scaled[k][lo:hi], onehots[k][lo:hi], down_weight)

    far1 = back(3, 0, half).astype(jnp.bfloat16)
    far2 = back(3, half, rows).astype(jnp.bfloat16)
    via1, via2 = over(far1, 1), over(far2, 2)
    got1a = over(back(1, 0, half).astype(jnp.bfloat16), 1)
    got2b = over(back(2, half, rows).astype(jnp.bfloat16), 2)
    near2 = (back(2, 0, half) + via1.astype(jnp.float32)).astype(jnp.bfloat16)
    near1 = (back(1, half, rows) + via2.astype(jnp.float32)).astype(jnp.bfloat16)
    got2a = [over(near2[i * cut : (i + 1) * cut], 2) for i in range(2)]
    got1b = [over(near1[i * cut : (i + 1) * cut], 1) for i in range(2)]
    base_a = back(0, 0, half)
    base_b = back(0, half, rows)

    kinds_all = jnp.stack(kinds)[None, :, None, :]
    down_grad = None
    for picked in ((0,), (1, 2)):
        labels = jnp.array(picked, jnp.int32)[:, None, None, None]
        marks = (kinds_all == labels).astype(jnp.float32)
        down_grad = weight_grad_of(
            picked, hidden, [scaled[k] for k in range(groups)], marks, down_grad
        )

    grads = None
    for base, direct, first, got, column in (
        (base_a, got1a, 0, got2a[0], 0),
        (base_b, got2b, 0, got1b[0], half),
        (base_a, got1a, cut, got2a[1], cut),
        (base_b, got2b, cut, got1b[1], half + cut),
    ):
        grads = grads_into(base.T, direct.T, first, got.T, gate_turned, up_turned, column, grads)
    gate_grad, up_grad = grads
    return (down_grad, gate_grad.T, up_grad.T)


def shards(modality, out_grad, gate_pre, up_pre, down_weight):
    rows, block = out_grad.shape
    groups = lax.axis_size("fsdp")
    lanes = lax.axis_size("tensor")
    width = down_weight.shape[2]
    me = lax.axis_index("fsdp")
    core = lax.axis_index("tensor") % 2
    pieces = width // (2 * block)

    cores = [[i for i in range(lanes) if i % 2 == c] for c in range(2)]
    stripe = lax.all_gather(out_grad, "tensor", axis=0, axis_index_groups=cores)
    stripe = stripe.reshape(groups, pieces, rows, block)

    hidden = hidden_of(gate_pre, up_pre)
    hid_list = [hidden] + [swap(hidden, "fsdp", groups, k) for k in range(1, groups)]

    kinds = lax.all_gather(modality, "fsdp", axis=0)
    counts = jnp.sum(kind_table(kinds.reshape(-1)), axis=0)
    factor = rows * groups / (3.0 * counts)

    order = [groups - 1] + list(range(1, groups - 1)) + [0]
    onehots, scaled = {}, {}
    for k in order:
        part = lax.dynamic_index_in_dim(stripe, me ^ k, 0, keepdims=False)
        if k:
            part = swap(part, "fsdp", groups, k)
        other = swap(part, "tensor", lanes, 1)
        first = jnp.where(core == 0, part, other)
        second = jnp.where(core == 0, other, part)
        joined = jnp.stack([first, second], axis=1).reshape(2 * pieces, rows, block)
        joined = jnp.concatenate([joined[i] for i in range(2 * pieces)], axis=1)
        onehots[k] = kind_table(lax.dynamic_index_in_dim(kinds, me ^ k, 0, keepdims=False))
        token_scale = jnp.sum(onehots[k] * factor[None, :], axis=1)
        scaled[k] = (joined.astype(jnp.float32) * token_scale[:, None]).astype(jnp.bfloat16)

    folded = masked_back(scaled[0], onehots[0], down_weight)
    for k in range(1, groups):
        sent = masked_back(scaled[k], onehots[k], down_weight).astype(jnp.bfloat16)
        folded = folded + swap(sent, "fsdp", groups, k).astype(jnp.float32)
    gate_grad, up_grad = grads_of(folded, gate_pre, up_pre)

    hid_all = jnp.concatenate(hid_list, axis=0)
    scaled_all = jnp.concatenate([scaled[k] for k in range(groups)], axis=0)
    onehot_all = jnp.concatenate([onehots[k] for k in range(groups)], axis=0)
    down_grad = weight_grad(hid_all, scaled_all, onehot_all)
    return (down_grad, gate_grad, up_grad)


def solution(mesh):
    placed = (
        P("fsdp"),
        P("fsdp", "tensor"),
        P("fsdp", "tensor"),
        P("fsdp", "tensor"),
        P(None, "tensor", "fsdp"),
    )
    square = mesh.shape["fsdp"] == 4 and mesh.shape["tensor"] == 8
    return jax.shard_map(
        shards_planes if square else shards,
        mesh=mesh,
        in_specs=placed,
        out_specs=(P(None, "tensor", "fsdp"), P("fsdp", "tensor"), P("fsdp", "tensor")),
        check_vma=False,
    )
```

```python
import functools

import jax
import jax.numpy as jnp
from jax import lax
from jax.experimental import pallas as pl
from jax.experimental.pallas import tpu as pltpu
from jax.sharding import PartitionSpec as P


def kind_table(kind_ids):
    labels = jnp.arange(3, dtype=jnp.int32)
    return (kind_ids[:, None] == labels[None, :]).astype(jnp.float32)


def swap(values, axis, size, step):
    return lax.ppermute(values, axis, [(i, i ^ step) for i in range(size)])


def activations(gate_pre, up_pre):
    gate_val = gate_pre.astype(jnp.float32)
    up_val = up_pre.astype(jnp.float32)
    sigmoid_g = jax.nn.sigmoid(gate_val)
    return gate_val, up_val, sigmoid_g, gate_val * sigmoid_g


def hidden_of(gate_pre, up_pre):
    _, up_val, _, active = activations(gate_pre, up_pre)
    return (active * up_val).astype(jnp.bfloat16)


def grads_of(folded, gate_pre, up_pre):
    gate_val, up_val, sigmoid_g, active = activations(gate_pre, up_pre)
    up_grad = (folded * active).astype(jnp.bfloat16)
    slope = sigmoid_g * (1.0 + gate_val * (1.0 - sigmoid_g))
    gate_grad = (folded * up_val * slope).astype(jnp.bfloat16)
    return gate_grad, up_grad


def masked_back(scaled, onehot, down_weight):
    marks = onehot.T.astype(jnp.bfloat16)
    masked = scaled[None, :, :] * marks[:, :, None]
    return lax.dot_general(
        masked, down_weight, (((0, 2), (0, 2)), ((), ())), preferred_element_type=jnp.float32
    )


def weight_grad(hid_all, scaled_all, onehot_all):
    marks_all = onehot_all.T.astype(jnp.bfloat16)
    masked_all = scaled_all[None, :, :] * marks_all[:, :, None]
    stacked = jnp.broadcast_to(hid_all[None, :, :], (3,) + hid_all.shape)
    return lax.dot_general(
        stacked, masked_all, (((1,), (1,)), ((0,), (0,))), preferred_element_type=jnp.float32
    )


HBM = pltpu.MemorySpace.HBM


def keep_body(source_ref, kept_ref, sem):
    copy = pltpu.make_async_copy(source_ref, kept_ref, sem)
    copy.start()
    copy.wait()


def keep_near(values):
    return pl.pallas_call(
        keep_body,
        out_shape=pltpu.VMEM(values.shape, values.dtype),
        in_specs=[pl.BlockSpec(memory_space=HBM)],
        out_specs=pl.BlockSpec(memory_space=pltpu.VMEM),
        scratch_shapes=[pltpu.SemaphoreType.DMA],
        compiler_params=pltpu.CompilerParams(vmem_limit_bytes=16 * 2**20),
    )(values)


def weight_body(kinds, owners, tile, *refs):
    pieces = refs[: sum(len(owner) for owner in owners)]
    scaled = refs[len(pieces) : len(pieces) + len(owners)]
    marks_ref = refs[len(pieces) + len(owners)]
    out_ref, hid_buf, scaled_buf, total, hid_sem, scaled_sem, out_sem = refs[-7:]
    chunks = len(owners)
    tiles = total.shape[1] // tile

    def fetch(at, slot, act):
        for c, owner in enumerate(owners):

            @pl.when(at == c)
            def _():
                act(pltpu.make_async_copy(scaled[c], scaled_buf.at[slot], scaled_sem.at[slot]))
                for p, (index, offset, count) in enumerate(owner):
                    here = hid_buf.at[slot, :, pl.ds(offset, count)]
                    act(pltpu.make_async_copy(pieces[index], here, hid_sem.at[slot, p]))

    fetch(0, 0, lambda copy: copy.start())

    def columns(t):
        return pl.ds(pl.multiple_of(t * tile, tile), tile)

    def put(n, t):
        return pltpu.make_async_copy(
            total.at[:, columns(t)], out_ref.at[kinds[0] + n, :, columns(t)], out_sem.at[t]
        )

    def chunk(step, carry):
        n, c = step // chunks, lax.rem(step, chunks)
        slot = lax.rem(step, 2)

        @pl.when(step + 1 < len(kinds) * chunks)
        def _():
            fetch(lax.rem(step + 1, chunks), 1 - slot, lambda copy: copy.start())

        fetch(c, slot, lambda copy: copy.wait())

        def one(t, carry):
            @pl.when((c == 0) & (n > 0))
            def _():
                put(n - 1, t).wait()

            mark = marks_ref[n, c].astype(jnp.bfloat16)
            part = jnp.dot(
                hid_buf[slot] * mark,
                scaled_buf[slot, :, columns(t)],
                preferred_element_type=jnp.float32,
            )
            total[:, columns(t)] = jnp.where(c > 0, total[:, columns(t)], 0.0) + part

            @pl.when(c == chunks - 1)
            def _():
                put(n, t).start()

            return carry

        return lax.fori_loop(0, tiles, one, carry)

    lax.fori_loop(0, len(kinds) * chunks, chunk, 0)
    for t in range(tiles):
        put(len(kinds) - 1, t).wait()


def weight_grad_of(kinds, hidden, scaled, marks, before):
    owners, pieces = [], []
    for owner in hidden:
        listed, offset = [], 0
        for piece in owner:
            listed.append((len(pieces), offset, piece.shape[1]))
            pieces.append(piece)
            offset += piece.shape[1]
        owners.append(tuple(listed))
    rows, cols = scaled[0].shape
    width = pieces[0].shape[0]
    tiles = 2
    hbm = pl.BlockSpec(memory_space=HBM)
    operands = [*pieces, *scaled, marks]
    specs = [hbm] * (len(operands) - 1) + [pl.BlockSpec(memory_space=pltpu.VMEM)]
    aliases = {}
    if before is not None:
        operands.append(before)
        specs.append(hbm)
        aliases = {len(operands) - 1: 0}
    most = max(len(owner) for owner in owners)
    tokens = rows * len(owners)
    return pl.pallas_call(
        functools.partial(weight_body, kinds, tuple(owners), cols // tiles),
        out_shape=jax.ShapeDtypeStruct((3, width, cols), jnp.float32),
        in_specs=specs,
        out_specs=hbm,
        scratch_shapes=[
            pltpu.VMEM((2, width, rows), jnp.bfloat16),
            pltpu.VMEM((2, rows, cols), jnp.bfloat16),
            pltpu.VMEM((width, cols), jnp.float32),
            pltpu.SemaphoreType.DMA((2, most)),
            pltpu.SemaphoreType.DMA((2,)),
            pltpu.SemaphoreType.DMA((tiles,)),
        ],
        input_output_aliases=aliases,
        compiler_params=pltpu.CompilerParams(vmem_limit_bytes=24 * 2**20),
        cost_estimate=pl.CostEstimate(
            flops=2 * len(kinds) * tokens * width * cols,
            bytes_accessed=2 * tokens * (width + cols) + 4 * len(kinds) * width * cols,
            transcendentals=0,
        ),
    )(*operands)


def grads_body(base_ref, direct_ref, got_ref, gate_ref, up_ref, *refs):
    gate_out, up_out = refs[-2:]
    count = got_ref.shape[1]
    lanes = 128 if count % 128 == 0 else count

    def one(j, carry):
        at = (slice(None), pl.ds(pl.multiple_of(j * lanes, lanes), lanes))
        folded = base_ref[at] + direct_ref[at].astype(jnp.float32) + got_ref[at].astype(jnp.float32)
        gate_out[at], up_out[at] = grads_of(folded, gate_ref[at], up_ref[at])
        return carry

    lax.fori_loop(0, count // lanes, one, 0)


def grads_into(base, direct, got, gate_turned, up_turned, column, before):
    width, count = got.shape
    steps = 4 if width % 64 == 0 else 1
    tall = width // steps

    def at(start):
        return pl.BlockSpec((tall, count), lambda i: (i, start // count))

    operands = [base, direct, got, gate_turned, up_turned]
    specs = [at(0), at(0), at(0), at(column), at(column)]
    aliases = {}
    if before is not None:
        operands += before
        specs += [pl.BlockSpec(memory_space=HBM)] * 2
        aliases = {5: 0, 6: 1}
    out = jax.ShapeDtypeStruct(gate_turned.shape, jnp.bfloat16)
    return pl.pallas_call(
        grads_body,
        grid=(steps,),
        out_shape=(out, out),
        in_specs=specs,
        out_specs=(at(column), at(column)),
        input_output_aliases=aliases,
        compiler_params=pltpu.CompilerParams(vmem_limit_bytes=16 * 2**20),
        cost_estimate=pl.CostEstimate(
            flops=20 * width * count,
            bytes_accessed=16 * width * count,
            transcendentals=width * count,
        ),
    )(*operands)


def shards_planes(modality, out_grad, gate_pre, up_pre, down_weight):
    return planes_body(modality, out_grad, gate_pre, up_pre, down_weight)


def planes_body(modality, out_grad, gate_pre, up_pre, down_weight):
    rows, block = out_grad.shape
    groups = lax.axis_size("fsdp")
    lanes = lax.axis_size("tensor")
    planes = lanes // 2
    quarter = rows // planes
    half = rows // 2
    me = lax.axis_index("fsdp")
    lane = lax.axis_index("tensor")
    plane = lane // 2
    core = lane % 2
    gate_turned, up_turned = gate_pre.T, up_pre.T

    def over(values, step):
        return lax.ppermute(values, "fsdp", [(i, i ^ step) for i in range(groups)])

    def along(values, step):
        return lax.ppermute(values, "tensor", [(i, i ^ step) for i in range(lanes)])

    hid_a = hidden_of(gate_turned[:, :half], up_turned[:, :half])
    hid_b = hidden_of(gate_turned[:, half:], up_turned[:, half:])
    hid1b, hid2a = over(hid_b, 1), over(hid_a, 2)
    hid1a, hid2b = over(hid_a, 1), over(hid_b, 2)
    hid3a, hid3b = over(hid2a, 1), over(hid1b, 2)
    hidden = [[hid_a, hid_b], [hid1a, hid1b], [hid2a, hid2b], [hid3a, hid3b]]

    own = out_grad.reshape(planes, quarter, block)
    legs = []
    for d in range(planes):
        part = lax.dynamic_index_in_dim(own, plane ^ d, 0, keepdims=False)
        legs.append(along(part, 2 * d) if d else part)

    kinds = [modality] + [over(modality, k) for k in range(1, groups)]

    stacked = jnp.stack(legs)
    crossed = {}
    for k in (3, 1, 2, 0):
        part = lax.dynamic_index_in_dim(stacked, plane ^ me ^ k, 0, keepdims=False)
        crossed[k] = over(part, k) if k else part

    onehots = [kind_table(kind_ids) for kind_ids in kinds]
    counts = sum(jnp.sum(onehot, axis=0) for onehot in onehots)
    factor = rows * groups / (3.0 * counts)

    odd = plane % 2 == 1
    upper = plane // 2 == 1
    inner = (plane == 1) | (plane == 2)
    middle = [(2 * p + c, 2 * (3 - p) + c) for p in (1, 2) for c in range(2)]
    outward = [(2 * p + c, 2 * (p ^ 1) + c) for p in (1, 2) for c in range(2)]
    scaled = {}
    for k in (0, 3, 1, 2):
        mine = crossed[k]
        near = along(mine, 2)
        pair = jnp.where(odd, jnp.concatenate([near, mine]), jnp.concatenate([mine, near]))
        across = lax.ppermute(pair, "tensor", middle)
        onward = lax.ppermute(across, "tensor", outward)
        beyond = jnp.where(inner, across, onward)
        part = jnp.where(upper, jnp.concatenate([beyond, pair]), jnp.concatenate([pair, beyond]))
        other = along(part, 1)
        joined = jnp.where(
            core == 0,
            jnp.concatenate([part, other], axis=1),
            jnp.concatenate([other, part], axis=1),
        )
        token_scale = jnp.sum(onehots[k] * factor[None, :], axis=1)
        scaled[k] = (joined.astype(jnp.float32) * token_scale[:, None]).astype(jnp.bfloat16)

    down_near = keep_near(down_weight)

    def back(k, lo, hi):
        return masked_back(scaled[k][lo:hi], onehots[k][lo:hi], down_near)

    far1 = back(3, 0, half).astype(jnp.bfloat16)
    far2 = back(3, half, rows).astype(jnp.bfloat16)
    via1, via2 = over(far1, 1), over(far2, 2)
    got1a = over(back(1, 0, half).astype(jnp.bfloat16), 1)
    got2b = over(back(2, half, rows).astype(jnp.bfloat16), 2)
    near2 = (back(2, 0, half) + via1.astype(jnp.float32)).astype(jnp.bfloat16)
    near1 = (back(1, half, rows) + via2.astype(jnp.float32)).astype(jnp.bfloat16)
    got2a, got1b = over(near2, 2), over(near1, 1)
    base_a = back(0, 0, half)
    base_b = back(0, half, rows)

    kinds_all = jnp.stack(kinds)[None, :, None, :]
    down_grad = None
    for picked in ((0, 1, 2),):
        labels = jnp.array(picked, jnp.int32)[:, None, None, None]
        marks = (kinds_all == labels).astype(jnp.float32)
        down_grad = weight_grad_of(
            picked, hidden, [scaled[k] for k in range(groups)], marks, down_grad
        )

    grads = None
    for base, direct, got, column in ((base_a, got1a, got2a, 0), (base_b, got2b, got1b, half)):
        grads = grads_into(base.T, direct.T, got.T, gate_turned, up_turned, column, grads)
    gate_grad, up_grad = grads
    return (down_grad, gate_grad.T, up_grad.T)


def shards(modality, out_grad, gate_pre, up_pre, down_weight):
    rows, block = out_grad.shape
    groups = lax.axis_size("fsdp")
    lanes = lax.axis_size("tensor")
    width = down_weight.shape[2]
    me = lax.axis_index("fsdp")
    core = lax.axis_index("tensor") % 2
    pieces = width // (2 * block)

    cores = [[i for i in range(lanes) if i % 2 == c] for c in range(2)]
    stripe = lax.all_gather(out_grad, "tensor", axis=0, axis_index_groups=cores)
    stripe = stripe.reshape(groups, pieces, rows, block)

    hidden = hidden_of(gate_pre, up_pre)
    hid_list = [hidden] + [swap(hidden, "fsdp", groups, k) for k in range(1, groups)]

    kinds = lax.all_gather(modality, "fsdp", axis=0)
    counts = jnp.sum(kind_table(kinds.reshape(-1)), axis=0)
    factor = rows * groups / (3.0 * counts)

    order = [groups - 1] + list(range(1, groups - 1)) + [0]
    onehots, scaled = {}, {}
    for k in order:
        part = lax.dynamic_index_in_dim(stripe, me ^ k, 0, keepdims=False)
        if k:
            part = swap(part, "fsdp", groups, k)
        other = swap(part, "tensor", lanes, 1)
        first = jnp.where(core == 0, part, other)
        second = jnp.where(core == 0, other, part)
        joined = jnp.stack([first, second], axis=1).reshape(2 * pieces, rows, block)
        joined = jnp.concatenate([joined[i] for i in range(2 * pieces)], axis=1)
        onehots[k] = kind_table(lax.dynamic_index_in_dim(kinds, me ^ k, 0, keepdims=False))
        token_scale = jnp.sum(onehots[k] * factor[None, :], axis=1)
        scaled[k] = (joined.astype(jnp.float32) * token_scale[:, None]).astype(jnp.bfloat16)

    folded = masked_back(scaled[0], onehots[0], down_weight)
    for k in range(1, groups):
        sent = masked_back(scaled[k], onehots[k], down_weight).astype(jnp.bfloat16)
        folded = folded + swap(sent, "fsdp", groups, k).astype(jnp.float32)
    gate_grad, up_grad = grads_of(folded, gate_pre, up_pre)

    hid_all = jnp.concatenate(hid_list, axis=0)
    scaled_all = jnp.concatenate([scaled[k] for k in range(groups)], axis=0)
    onehot_all = jnp.concatenate([onehots[k] for k in range(groups)], axis=0)
    down_grad = weight_grad(hid_all, scaled_all, onehot_all)
    return (down_grad, gate_grad, up_grad)


def solution(mesh):
    placed = (
        P("fsdp"),
        P("fsdp", "tensor"),
        P("fsdp", "tensor"),
        P("fsdp", "tensor"),
        P(None, "tensor", "fsdp"),
    )
    square = mesh.shape["fsdp"] == 4 and mesh.shape["tensor"] == 8
    return jax.shard_map(
        shards_planes if square else shards,
        mesh=mesh,
        in_specs=placed,
        out_specs=(P(None, "tensor", "fsdp"), P("fsdp", "tensor"), P("fsdp", "tensor")),
        check_vma=False,
    )
```

```python
import functools

import jax
import jax.numpy as jnp
from jax import lax
from jax.experimental import pallas as pl
from jax.experimental.pallas import tpu as pltpu
from jax.sharding import PartitionSpec as P


def kind_table(kind_ids):
    labels = jnp.arange(3, dtype=jnp.int32)
    return (kind_ids[:, None] == labels[None, :]).astype(jnp.float32)


def swap(values, axis, size, step):
    return lax.ppermute(values, axis, [(i, i ^ step) for i in range(size)])


def activations(gate_pre, up_pre):
    gate_val = gate_pre.astype(jnp.float32)
    up_val = up_pre.astype(jnp.float32)
    sigmoid_g = 0.5 * jnp.tanh(0.5 * gate_val) + 0.5
    return gate_val, up_val, sigmoid_g, gate_val * sigmoid_g


def hidden_of(gate_pre, up_pre):
    _, up_val, _, active = activations(gate_pre, up_pre)
    return (active * up_val).astype(jnp.bfloat16)


def grads_of(folded, gate_pre, up_pre):
    _, up_val, sigmoid_g, active = activations(gate_pre, up_pre)
    up_grad = (folded * active).astype(jnp.bfloat16)
    slope = sigmoid_g + active * (1.0 - sigmoid_g)
    gate_grad = (folded * up_val * slope).astype(jnp.bfloat16)
    return gate_grad, up_grad


def masked_back(scaled, onehot, down_weight):
    marks = onehot.T.astype(jnp.bfloat16)
    masked = scaled[None, :, :] * marks[:, :, None]
    return lax.dot_general(
        masked, down_weight, (((0, 2), (0, 2)), ((), ())), preferred_element_type=jnp.float32
    )


def weight_grad(hid_all, scaled_all, onehot_all):
    marks_all = onehot_all.T.astype(jnp.bfloat16)
    masked_all = scaled_all[None, :, :] * marks_all[:, :, None]
    stacked = jnp.broadcast_to(hid_all[None, :, :], (3,) + hid_all.shape)
    return lax.dot_general(
        stacked, masked_all, (((1,), (1,)), ((0,), (0,))), preferred_element_type=jnp.float32
    )


HBM = pltpu.MemorySpace.HBM


def keep_body(source_ref, kept_ref, sem):
    copy = pltpu.make_async_copy(source_ref, kept_ref, sem)
    copy.start()
    copy.wait()


def keep_near(values):
    return pl.pallas_call(
        keep_body,
        out_shape=pltpu.VMEM(values.shape, values.dtype),
        in_specs=[pl.BlockSpec(memory_space=HBM)],
        out_specs=pl.BlockSpec(memory_space=pltpu.VMEM),
        scratch_shapes=[pltpu.SemaphoreType.DMA],
        compiler_params=pltpu.CompilerParams(vmem_limit_bytes=16 * 2**20),
    )(values)


def weight_body(kinds, owners, tile, *refs):
    pieces = refs[: sum(len(owner) for owner in owners)]
    scaled = refs[len(pieces) : len(pieces) + len(owners)]
    marks_ref = refs[len(pieces) + len(owners)]
    out_ref, hid_buf, scaled_buf, total, hid_sem, scaled_sem, out_sem = refs[-7:]
    chunks = len(owners)
    tiles = total.shape[1] // tile

    def fetch(at, slot, act):
        for c, owner in enumerate(owners):

            @pl.when(at == c)
            def _():
                act(pltpu.make_async_copy(scaled[c], scaled_buf.at[slot], scaled_sem.at[slot]))
                for p, (index, offset, count) in enumerate(owner):
                    here = hid_buf.at[slot, :, pl.ds(offset, count)]
                    act(pltpu.make_async_copy(pieces[index], here, hid_sem.at[slot, p]))

    fetch(0, 0, lambda copy: copy.start())

    def columns(t):
        return pl.ds(pl.multiple_of(t * tile, tile), tile)

    def put(n, t):
        return pltpu.make_async_copy(
            total.at[:, columns(t)], out_ref.at[kinds[0] + n, :, columns(t)], out_sem.at[t]
        )

    def chunk(step, carry):
        n, c = step // chunks, lax.rem(step, chunks)
        slot = lax.rem(step, 2)

        @pl.when(step + 1 < len(kinds) * chunks)
        def _():
            fetch(lax.rem(step + 1, chunks), 1 - slot, lambda copy: copy.start())

        fetch(c, slot, lambda copy: copy.wait())

        def one(t, carry):
            @pl.when((c == 0) & (n > 0))
            def _():
                put(n - 1, t).wait()

            mark = marks_ref[n, c].astype(jnp.bfloat16)
            part = jnp.dot(
                hid_buf[slot] * mark,
                scaled_buf[slot, :, columns(t)],
                preferred_element_type=jnp.float32,
            )
            total[:, columns(t)] = jnp.where(c > 0, total[:, columns(t)], 0.0) + part

            @pl.when(c == chunks - 1)
            def _():
                put(n, t).start()

            return carry

        return lax.fori_loop(0, tiles, one, carry)

    lax.fori_loop(0, len(kinds) * chunks, chunk, 0)
    for t in range(tiles):
        put(len(kinds) - 1, t).wait()


def weight_grad_of(kinds, hidden, scaled, marks, before):
    owners, pieces = [], []
    for owner in hidden:
        listed, offset = [], 0
        for piece in owner:
            listed.append((len(pieces), offset, piece.shape[1]))
            pieces.append(piece)
            offset += piece.shape[1]
        owners.append(tuple(listed))
    rows, cols = scaled[0].shape
    width = pieces[0].shape[0]
    tiles = 2
    hbm = pl.BlockSpec(memory_space=HBM)
    operands = [*pieces, *scaled, marks]
    specs = [hbm] * (len(operands) - 1) + [pl.BlockSpec(memory_space=pltpu.VMEM)]
    aliases = {}
    if before is not None:
        operands.append(before)
        specs.append(hbm)
        aliases = {len(operands) - 1: 0}
    most = max(len(owner) for owner in owners)
    tokens = rows * len(owners)
    return pl.pallas_call(
        functools.partial(weight_body, kinds, tuple(owners), cols // tiles),
        out_shape=jax.ShapeDtypeStruct((3, width, cols), jnp.float32),
        in_specs=specs,
        out_specs=hbm,
        scratch_shapes=[
            pltpu.VMEM((2, width, rows), jnp.bfloat16),
            pltpu.VMEM((2, rows, cols), jnp.bfloat16),
            pltpu.VMEM((width, cols), jnp.float32),
            pltpu.SemaphoreType.DMA((2, most)),
            pltpu.SemaphoreType.DMA((2,)),
            pltpu.SemaphoreType.DMA((tiles,)),
        ],
        input_output_aliases=aliases,
        compiler_params=pltpu.CompilerParams(vmem_limit_bytes=24 * 2**20),
        cost_estimate=pl.CostEstimate(
            flops=2 * len(kinds) * tokens * width * cols,
            bytes_accessed=2 * tokens * (width + cols) + 4 * len(kinds) * width * cols,
            transcendentals=0,
        ),
    )(*operands)


def grads_body(base_ref, direct_ref, got_ref, gate_ref, up_ref, *refs):
    gate_out, up_out = refs[-2:]
    count = got_ref.shape[1]
    lanes = 128 if count % 128 == 0 else count

    def one(j, carry):
        at = (slice(None), pl.ds(pl.multiple_of(j * lanes, lanes), lanes))
        folded = base_ref[at] + direct_ref[at].astype(jnp.float32) + got_ref[at].astype(jnp.float32)
        gate_out[at], up_out[at] = grads_of(folded, gate_ref[at], up_ref[at])
        return carry

    lax.fori_loop(0, count // lanes, one, 0)


def grads_into(base, direct, got, gate_turned, up_turned, column, before):
    width, count = got.shape
    steps = 4 if width % 64 == 0 else 1
    tall = width // steps

    def at(start):
        return pl.BlockSpec((tall, count), lambda i: (i, start // count))

    operands = [base, direct, got, gate_turned, up_turned]
    specs = [at(0), at(0), at(0), at(column), at(column)]
    aliases = {}
    if before is not None:
        operands += before
        specs += [pl.BlockSpec(memory_space=HBM)] * 2
        aliases = {5: 0, 6: 1}
    out = jax.ShapeDtypeStruct(gate_turned.shape, jnp.bfloat16)
    return pl.pallas_call(
        grads_body,
        grid=(steps,),
        out_shape=(out, out),
        in_specs=specs,
        out_specs=(at(column), at(column)),
        input_output_aliases=aliases,
        compiler_params=pltpu.CompilerParams(vmem_limit_bytes=16 * 2**20),
        cost_estimate=pl.CostEstimate(
            flops=20 * width * count,
            bytes_accessed=16 * width * count,
            transcendentals=width * count,
        ),
    )(*operands)


def shards_planes(modality, out_grad, gate_pre, up_pre, down_weight):
    return planes_body(modality, out_grad, gate_pre, up_pre, down_weight)


def planes_body(modality, out_grad, gate_pre, up_pre, down_weight):
    rows, block = out_grad.shape
    groups = lax.axis_size("fsdp")
    lanes = lax.axis_size("tensor")
    planes = lanes // 2
    quarter = rows // planes
    half = rows // 2
    me = lax.axis_index("fsdp")
    lane = lax.axis_index("tensor")
    plane = lane // 2
    core = lane % 2
    gate_turned, up_turned = gate_pre.T, up_pre.T

    def over(values, step):
        return lax.ppermute(values, "fsdp", [(i, i ^ step) for i in range(groups)])

    def along(values, step):
        return lax.ppermute(values, "tensor", [(i, i ^ step) for i in range(lanes)])

    hid_a = hidden_of(gate_turned[:, :half], up_turned[:, :half])
    hid_b = hidden_of(gate_turned[:, half:], up_turned[:, half:])
    hid1b, hid2a = over(hid_b, 1), over(hid_a, 2)
    hid1a, hid2b = over(hid_a, 1), over(hid_b, 2)
    hid3a, hid3b = over(hid2a, 1), over(hid1b, 2)
    hidden = [[hid_a, hid_b], [hid1a, hid1b], [hid2a, hid2b], [hid3a, hid3b]]

    own = out_grad.reshape(planes, quarter, block)
    legs = []
    for d in range(planes):
        part = lax.dynamic_index_in_dim(own, plane ^ d, 0, keepdims=False)
        legs.append(along(part, 2 * d) if d else part)

    kinds = [modality] + [over(modality, k) for k in range(1, groups)]

    stacked = jnp.stack(legs)
    crossed = {}
    for k in (3, 1, 2, 0):
        part = lax.dynamic_index_in_dim(stacked, plane ^ me ^ k, 0, keepdims=False)
        crossed[k] = over(part, k) if k else part

    onehots = [kind_table(kind_ids) for kind_ids in kinds]
    counts = sum(jnp.sum(onehot, axis=0) for onehot in onehots)
    factor = rows * groups / (3.0 * counts)

    odd = plane % 2 == 1
    upper = plane // 2 == 1
    inner = (plane == 1) | (plane == 2)
    middle = [(2 * p + c, 2 * (3 - p) + c) for p in (1, 2) for c in range(2)]
    outward = [(2 * p + c, 2 * (p ^ 1) + c) for p in (1, 2) for c in range(2)]
    scaled = {}
    for k in (0, 3, 1, 2):
        mine = crossed[k]
        near = along(mine, 2)
        pair = jnp.where(odd, jnp.concatenate([near, mine]), jnp.concatenate([mine, near]))
        across = lax.ppermute(pair, "tensor", middle)
        onward = lax.ppermute(across, "tensor", outward)
        beyond = jnp.where(inner, across, onward)
        part = jnp.where(upper, jnp.concatenate([beyond, pair]), jnp.concatenate([pair, beyond]))
        other = along(part, 1)
        joined = jnp.where(
            core == 0,
            jnp.concatenate([part, other], axis=1),
            jnp.concatenate([other, part], axis=1),
        )
        token_scale = jnp.sum(onehots[k] * factor[None, :], axis=1)
        scaled[k] = (joined.astype(jnp.float32) * token_scale[:, None]).astype(jnp.bfloat16)

    down_near = keep_near(down_weight)

    def back(k, lo, hi):
        return masked_back(scaled[k][lo:hi], onehots[k][lo:hi], down_near)

    far1 = back(3, 0, half).astype(jnp.bfloat16)
    far2 = back(3, half, rows).astype(jnp.bfloat16)
    via1, via2 = over(far1, 1), over(far2, 2)
    got1a = over(back(1, 0, half).astype(jnp.bfloat16), 1)
    got2b = over(back(2, half, rows).astype(jnp.bfloat16), 2)
    near2 = (back(2, 0, half) + via1.astype(jnp.float32)).astype(jnp.bfloat16)
    near1 = (back(1, half, rows) + via2.astype(jnp.float32)).astype(jnp.bfloat16)
    got2a, got1b = over(near2, 2), over(near1, 1)
    base_a = back(0, 0, half)
    base_b = back(0, half, rows)

    kinds_all = jnp.stack(kinds)[None, :, None, :]
    down_grad = None
    for picked in ((0, 1, 2),):
        labels = jnp.array(picked, jnp.int32)[:, None, None, None]
        marks = (kinds_all == labels).astype(jnp.float32)
        down_grad = weight_grad_of(
            picked, hidden, [scaled[k] for k in range(groups)], marks, down_grad
        )

    grads = None
    for base, direct, got, column in ((base_a, got1a, got2a, 0), (base_b, got2b, got1b, half)):
        grads = grads_into(base.T, direct.T, got.T, gate_turned, up_turned, column, grads)
    gate_grad, up_grad = grads
    return (down_grad, gate_grad.T, up_grad.T)


def shards(modality, out_grad, gate_pre, up_pre, down_weight):
    rows, block = out_grad.shape
    groups = lax.axis_size("fsdp")
    lanes = lax.axis_size("tensor")
    width = down_weight.shape[2]
    me = lax.axis_index("fsdp")
    core = lax.axis_index("tensor") % 2
    pieces = width // (2 * block)

    cores = [[i for i in range(lanes) if i % 2 == c] for c in range(2)]
    stripe = lax.all_gather(out_grad, "tensor", axis=0, axis_index_groups=cores)
    stripe = stripe.reshape(groups, pieces, rows, block)

    hidden = hidden_of(gate_pre, up_pre)
    hid_list = [hidden] + [swap(hidden, "fsdp", groups, k) for k in range(1, groups)]

    kinds = lax.all_gather(modality, "fsdp", axis=0)
    counts = jnp.sum(kind_table(kinds.reshape(-1)), axis=0)
    factor = rows * groups / (3.0 * counts)

    order = [groups - 1] + list(range(1, groups - 1)) + [0]
    onehots, scaled = {}, {}
    for k in order:
        part = lax.dynamic_index_in_dim(stripe, me ^ k, 0, keepdims=False)
        if k:
            part = swap(part, "fsdp", groups, k)
        other = swap(part, "tensor", lanes, 1)
        first = jnp.where(core == 0, part, other)
        second = jnp.where(core == 0, other, part)
        joined = jnp.stack([first, second], axis=1).reshape(2 * pieces, rows, block)
        joined = jnp.concatenate([joined[i] for i in range(2 * pieces)], axis=1)
        onehots[k] = kind_table(lax.dynamic_index_in_dim(kinds, me ^ k, 0, keepdims=False))
        token_scale = jnp.sum(onehots[k] * factor[None, :], axis=1)
        scaled[k] = (joined.astype(jnp.float32) * token_scale[:, None]).astype(jnp.bfloat16)

    folded = masked_back(scaled[0], onehots[0], down_weight)
    for k in range(1, groups):
        sent = masked_back(scaled[k], onehots[k], down_weight).astype(jnp.bfloat16)
        folded = folded + swap(sent, "fsdp", groups, k).astype(jnp.float32)
    gate_grad, up_grad = grads_of(folded, gate_pre, up_pre)

    hid_all = jnp.concatenate(hid_list, axis=0)
    scaled_all = jnp.concatenate([scaled[k] for k in range(groups)], axis=0)
    onehot_all = jnp.concatenate([onehots[k] for k in range(groups)], axis=0)
    down_grad = weight_grad(hid_all, scaled_all, onehot_all)
    return (down_grad, gate_grad, up_grad)


def solution(mesh):
    placed = (
        P("fsdp"),
        P("fsdp", "tensor"),
        P("fsdp", "tensor"),
        P("fsdp", "tensor"),
        P(None, "tensor", "fsdp"),
    )
    square = mesh.shape["fsdp"] == 4 and mesh.shape["tensor"] == 8
    return jax.shard_map(
        shards_planes if square else shards,
        mesh=mesh,
        in_specs=placed,
        out_specs=(P(None, "tensor", "fsdp"), P("fsdp", "tensor"), P("fsdp", "tensor")),
        check_vma=False,
    )
```
